32 devices in a mesh: fsdp: 4 (over z), ep: 8 (over y, x, core).
Axes of the slice: x: 2, y: 2, z: 4, core: 2. Of those that a mesh axis runs over, the one named last changes fastest.
Arguments:
- x_in: bfloat16 [2, 32768, 512], P(None, ('fsdp', 'ep'))
- dy_out: bfloat16 [2, 32768, 512], P(None, ('fsdp', 'ep'))
- expert_idx: int32 [2, 32768, 8], P(None, ('fsdp', 'ep'))
- gate_prob: float32 [2, 32768, 8], P(None, ('fsdp', 'ep'))
- w_one: bfloat16 [64, 512, 256], P('ep', 'fsdp')
- w_two: bfloat16 [64, 256, 512], P('ep', None, 'fsdp')
- w_three: bfloat16 [64, 512, 256], P('ep', 'fsdp')
Outputs:
- output 1: bfloat16 [2, 32768, 512], P(None, ('fsdp', 'ep'))
- output 2: float32 [2, 32768, 8], P(None, ('fsdp', 'ep'))
- output 3: float32 [64, 512, 256], P('ep', 'fsdp')
- output 4: float32 [64, 256, 512], P('ep', None, 'fsdp')
- output 5: float32 [64, 512, 256], P('ep', 'fsdp')
All inputs are finite; a program needn't handle non-finite values.
Results may differ from the reference program's by a relative error of at most 0.001.
Values are sent between devices in bfloat16 or wider.
A program may use at most 1 GiB of HBM per device.

```python
import jax
import jax.numpy as jnp
from jax import lax

D_MODEL = 512
FF_DIM = 256
EXPERTS = 64
TOP_K = 8
TOK_DEV = 1024
SOURCES = 32
MICRO_BATCHES = 2
CAPACITY = 160

TOKENS = SOURCES * TOK_DEV
N_CHOICE = TOK_DEV * TOP_K


def draw_routing(key):
    key_hot, key_bias, key_score = jax.random.split(key, 3)
    expert_ids = jnp.arange(EXPERTS, dtype=jnp.int32)
    hot_ids = jax.random.randint(key_hot, (MICRO_BATCHES, SOURCES, 1, 1), 0, EXPERTS)
    forced = jnp.arange(TOK_DEV)[:, None] < CAPACITY
    hot_bonus = jnp.where(expert_ids == hot_ids, 1, 0) * jnp.where(forced, 4096, 512)
    source_bias = jax.random.randint(key_bias, (MICRO_BATCHES, SOURCES, 1, EXPERTS), 0, 512)
    rand_score = jax.random.randint(key_score, (MICRO_BATCHES, SOURCES, TOK_DEV, EXPERTS), 0, 1024)
    total_score = (rand_score + source_bias + hot_bonus) * EXPERTS + expert_ids
    chosen = lax.top_k(total_score, TOP_K)[1]
    return chosen.reshape(MICRO_BATCHES, TOKENS, TOP_K).astype(jnp.int32)


def setup_inputs(seed: int = 0) -> dict:
    key_list = jax.random.split(jax.random.key(seed), 7)
    x_vals = jax.random.normal(key_list[0], (MICRO_BATCHES, TOKENS, D_MODEL), jnp.float32)
    dy_vals = jax.random.normal(key_list[1], (MICRO_BATCHES, TOKENS, D_MODEL), jnp.float32)
    routing = draw_routing(key_list[2])
    gate_vals = jax.random.uniform(key_list[3], (MICRO_BATCHES, TOKENS, TOP_K), jnp.float32, 0.2, 1.0)
    w_one = jax.random.normal(key_list[4], (EXPERTS, D_MODEL, FF_DIM), jnp.float32) * D_MODEL ** -0.5
    w_two = jax.random.normal(key_list[5], (EXPERTS, FF_DIM, D_MODEL), jnp.float32) * FF_DIM ** -0.5
    w_three = jax.random.normal(key_list[6], (EXPERTS, D_MODEL, FF_DIM), jnp.float32) * D_MODEL ** -0.5
    return {'x_in': x_vals.astype(jnp.bfloat16), 'dy_out': dy_vals.astype(jnp.bfloat16), 'expert_idx': routing, 'gate_prob': gate_vals, 'w_one': w_one.astype(jnp.bfloat16), 'w_two': w_two.astype(jnp.bfloat16), 'w_three': w_three.astype(jnp.bfloat16)}


def slot_holder(ids_flat):
    one_hot = (ids_flat[:, None] == jnp.arange(EXPERTS, dtype=jnp.int32)[None, :]).astype(jnp.int32)
    position = jnp.sum((jnp.cumsum(one_hot, axis=0) - one_hot) * one_hot, axis=1)
    choice_slot = jnp.where(position < CAPACITY, ids_flat * CAPACITY + position, EXPERTS * CAPACITY)
    holder = jnp.full((EXPERTS * CAPACITY + 1,), N_CHOICE, jnp.int32)
    holder = holder.at[choice_slot].set(jnp.arange(N_CHOICE, dtype=jnp.int32))
    return holder[:EXPERTS * CAPACITY]


def expert_rows(x_rows, dy_rows, gate_rows, w_a, w_b, w_c):
    h_one = jnp.dot(x_rows, w_a, preferred_element_type=jnp.float32)
    h_three = jnp.dot(x_rows, w_c, preferred_element_type=jnp.float32)
    sigma_one = jax.nn.sigmoid(h_one)
    silu_one = h_one * sigma_one
    act_bf = (silu_one * h_three).astype(jnp.bfloat16)
    y_rows = jnp.dot(act_bf, w_b, preferred_element_type=jnp.float32)
    dg_rows = jnp.sum(dy_rows.astype(jnp.float32) * y_rows, axis=1)
    g_rows = (gate_rows[:, None] * dy_rows.astype(jnp.float32)).astype(jnp.bfloat16)
    d_act = jnp.dot(g_rows, w_b.T, preferred_element_type=jnp.float32)
    dh_three = (d_act * silu_one).astype(jnp.bfloat16)
    dh_one = (d_act * h_three * sigma_one * (1.0 + h_one * (1.0 - sigma_one))).astype(jnp.bfloat16)
    dx_rows = (jnp.dot(dh_one, w_a.T, preferred_element_type=jnp.float32) + jnp.dot(dh_three, w_c.T, preferred_element_type=jnp.float32)).astype(jnp.bfloat16)
    gw_one = jnp.dot(x_rows.T, dh_one, preferred_element_type=jnp.float32)
    gw_two = jnp.dot(act_bf.T, g_rows, preferred_element_type=jnp.float32)
    gw_three = jnp.dot(x_rows.T, dh_three, preferred_element_type=jnp.float32)
    return dx_rows, dg_rows, gw_one, gw_two, gw_three


def reference(x_in, dy_out, expert_idx, gate_prob, w_one, w_two, w_three):
    total_choices = MICRO_BATCHES * TOKENS * TOP_K
    holder = lax.map(slot_holder, expert_idx.reshape(MICRO_BATCHES * SOURCES, N_CHOICE))
    block_base = jnp.arange(MICRO_BATCHES * SOURCES, dtype=jnp.int32)[:, None] * N_CHOICE
    slot_choice = jnp.where(holder < N_CHOICE, holder + block_base, total_choices)
    slot_choice = jnp.transpose(slot_choice.reshape(MICRO_BATCHES, SOURCES, EXPERTS, CAPACITY), (2, 0, 1, 3))
    slot_choice = slot_choice.reshape(EXPERTS, MICRO_BATCHES, SOURCES * CAPACITY)
    zero_row = jnp.zeros((1, D_MODEL), x_in.dtype)
    x_flat = jnp.concatenate([x_in.reshape(MICRO_BATCHES * TOKENS, D_MODEL), zero_row], axis=0)
    dy_flat = jnp.concatenate([dy_out.reshape(MICRO_BATCHES * TOKENS, D_MODEL), zero_row], axis=0)
    gate_flat = jnp.concatenate([gate_prob.reshape(total_choices), jnp.zeros((1,), gate_prob.dtype)])

    def expert_step(scan_state, per_expert):
        dx_acc, dg_acc = scan_state
        w_a, w_b, w_c, choices = per_expert
        grad_one = jnp.zeros((D_MODEL, FF_DIM), jnp.float32)
        grad_two = jnp.zeros((FF_DIM, D_MODEL), jnp.float32)
        grad_three = jnp.zeros((D_MODEL, FF_DIM), jnp.float32)
        for mb_index in range(MICRO_BATCHES):
            pick_ids = choices[mb_index]
            tok_ids = pick_ids // TOP_K
            dx_rows, dg_rows, gw_one, gw_two, gw_three = expert_rows(x_flat[tok_ids], dy_flat[tok_ids], gate_flat[pick_ids], w_a, w_b, w_c)
            dx_acc = dx_acc.at[tok_ids].add(dx_rows.astype(jnp.float32))
            dg_acc = dg_acc.at[pick_ids].set(dg_rows)
            grad_one = grad_one + gw_one
            grad_two = grad_two + gw_two
            grad_three = grad_three + gw_three
        return (dx_acc, dg_acc), (grad_one, grad_two, grad_three)

    start_state = (jnp.zeros((MICRO_BATCHES * TOKENS + 1, D_MODEL), jnp.float32), jnp.zeros((total_choices + 1,), jnp.float32))
    end_state, grad_stack = lax.scan(expert_step, start_state, (w_one, w_two, w_three, slot_choice))
    dx_in = end_state[0][:MICRO_BATCHES * TOKENS].astype(jnp.bfloat16).reshape(MICRO_BATCHES, TOKENS, D_MODEL)
    d_gate = end_state[1][:total_choices].reshape(MICRO_BATCHES, TOKENS, TOP_K)
    return (dx_in, d_gate, grad_stack[0], grad_stack[1], grad_stack[2])
```

```python
import functools

import jax
import jax.numpy as jnp
from jax import lax
from jax.experimental import pallas as pl
from jax.experimental.pallas import tpu as pltpu
from jax.sharding import PartitionSpec as P

MESH = pl.DeviceIdType.MESH
BF = jnp.bfloat16
F32 = jnp.float32
ANY = pl.BlockSpec(memory_space=pl.ANY)
VM = pl.BlockSpec(memory_space=pltpu.VMEM)
VLIM = 62 * 1024 * 1024
GROUPS = (1, 3, 4)
DROPPED = -4096.0
LANES = 128
EXP = 8
NT = (((1,), (1,)), ((), ()))
TN = (((0,), (0,)), ((), ()))


def params(collective_id=None):
    if collective_id is None:
        return pltpu.CompilerParams(vmem_limit_bytes=VLIM)
    return pltpu.CompilerParams(collective_id=collective_id, has_side_effects=True, vmem_limit_bytes=VLIM)


def cost(gflop, mbytes):
    return pl.CostEstimate(flops=gflop * 10**9, bytes_accessed=mbytes * 10**6, transcendentals=0)


def capacity_of(tok_rows, top_k, experts):
    return 8 * ((5 * tok_rows * top_k + 32 * experts - 1) // (32 * experts))


def dot(a, b):
    return jnp.dot(a, b, preferred_element_type=F32)


def hot_bf(sel):
    return jnp.where(sel, 1.0, 0.0).astype(BF)


def iota(shape, dim):
    return lax.broadcasted_iota(jnp.int32, shape, dim).astype(F32)


class Place:
    def __init__(self):
        me = lax.axis_index('ep')
        z = lax.axis_index('fsdp')
        self.me = me
        self.core = lax.rem(me, 2)
        self.other = 1 - self.core
        self.partner = me + 1 - 2 * self.core
        self.chip = lax.div(me, 2)
        self.to_x = 1 - 2 * lax.rem(self.chip, 2)
        self.to_y = 2 - 4 * lax.div(self.chip, 2)
        self.chip_x = self.chip + self.to_x
        self.chip_y = self.chip + self.to_y
        self.chip_d = self.chip_x + self.to_y
        self.dev_x = (z, 2 * self.chip_x + self.core)
        self.dev_y = (z, 2 * self.chip_y + self.core)
        self.dev_c = (z, self.partner)

    def greet(self):
        barrier = pltpu.get_barrier_semaphore()
        devices = (self.dev_x, self.dev_y, self.dev_c)
        for dev in devices:
            pl.semaphore_signal(barrier, inc=1, device_id=dev, device_id_type=MESH)
        pl.semaphore_wait(barrier, len(devices))


def rcopy(src, dst, sems, i, dev):
    return pltpu.make_async_remote_copy(src_ref=src, dst_ref=dst, send_sem=sems[0].at[i], recv_sem=sems[1].at[i], device_id=dev, device_id_type=MESH)


def arrive(ref, sems, i, dev):
    rcopy(ref, ref, sems, i, dev).wait_recv()


def gather_rows_kernel(capacity, x_ref, dy_ref, meta_ref, rows, pos_ref, gate_ref, post_ref, ids_ref, tg, mg, hot_a, hot_b, tri, stage, s_x, r_x, s_y, r_y, s_c, r_c, s_ax, r_ax, s_ay, r_ay, s_fx, r_fx, s_fy, r_fy, s_fa, r_fa, s_fb, r_fb, s_l, s_s):
    at = Place()
    tok = x_ref.shape[1]
    half = tok // 2
    by_x, by_y, by_c, relay_x, relay_y = (s_x, r_x), (s_y, r_y), (s_c, r_c), (s_ax, r_ax), (s_ay, r_ay)
    fwd_x, fwd_y, fwd_a, fwd_b = (s_fx, r_fx), (s_fy, r_fy), (s_fa, r_fa), (s_fb, r_fb)
    chunks = range(5)

    def slot_of(core, chip):
        return core * 4 + chip

    def own(k):
        if k == 0:
            return meta_ref
        return (dy_ref, x_ref)[k % 2].at[(k - 1) // 2]

    def block(k, slot):
        if k == 0:
            return mg.at[slot]
        return tg.at[(k - 1) % 2, slot, (k - 1) // 2]

    def part(k, slot, h):
        if k == 0:
            return mg.at[slot, h]
        return block(k, slot).at[pl.ds(h * half, half)]

    slot = slot_of(at.core, at.chip)
    slot_x = slot_of(at.core, at.chip_x)
    slot_y = slot_of(at.core, at.chip_y)
    slot_d = slot_of(at.core, at.chip_d)

    def side_hops(k):
        return (
            (part(k, slot_x, 0), part(k, slot_x, 0), relay_y, k, at.dev_y),
            (block(k, slot_x), block(k, slot_x), fwd_x, k, at.dev_c),
            (part(k, slot_y, 1), part(k, slot_y, 1), relay_x, k, at.dev_x),
            (block(k, slot_y), block(k, slot_y), fwd_y, k, at.dev_c),
        )

    def corner_hops(k):
        return ((part(k, slot_d, 0), part(k, slot_d, 0), fwd_a, k, at.dev_c), (part(k, slot_d, 1), part(k, slot_d, 1), fwd_b, k, at.dev_c))

    def own_hops(k):
        return tuple((own(k), block(k, slot), sems, k, dev) for sems, dev in ((by_x, at.dev_x), (by_y, at.dev_y), (by_c, at.dev_c)))

    def send(hops):
        for hop in hops:
            rcopy(*hop).start()

    def pass_on(k):
        hops = side_hops(k)
        arrive(block(k, slot_x), by_x, k, at.dev_x)
        send(hops[:2])
        arrive(block(k, slot_y), by_y, k, at.dev_y)
        send(hops[2:])
        arrive(block(k, slot_of(at.other, at.chip_x)), fwd_x, k, at.dev_c)
        arrive(block(k, slot_of(at.other, at.chip_y)), fwd_y, k, at.dev_c)

    def pass_on_corner(k):
        hops = corner_hops(k)
        far = slot_of(at.other, at.chip_d)
        arrive(part(k, slot_d, 0), relay_y, k, at.dev_y)
        send(hops[:1])
        arrive(part(k, slot_d, 1), relay_x, k, at.dev_x)
        send(hops[1:])
        arrive(part(k, far, 0), fwd_a, k, at.dev_c)
        arrive(part(k, far, 1), fwd_b, k, at.dev_c)

    local = [pltpu.make_async_copy(own(k), block(k, slot), s_l.at[k]) for k in chunks]
    for copy in local:
        copy.start()
    at.greet()
    for k in chunks:
        send(own_hops(k)[:2])
    for k in chunks:
        send(own_hops(k)[2:])

    tri[...] = hot_bf(iota((tok, tok), 0) < iota((tok, tok), 1))
    for copy in local:
        copy.wait()
    arrive(block(0, slot_of(at.other, at.chip)), by_c, 0, at.dev_c)
    pass_on(0)
    pass_on_corner(0)
    sub = iota((EXP, tok), 0)

    def hot_of(src, mb, device):
        ids = mg[src, 0, mb]
        vals = mg[src, 1, mb]
        want = sub + (device * EXP).astype(F32)
        hot = jnp.zeros((EXP, tok), F32)
        gate = hot
        for j in range(ids.shape[0]):
            sel = ids[j:j + 1, :] == want
            hot = jnp.where(sel, 1.0, hot)
            gate = jnp.where(sel, vals[j:j + 1, :], gate)
        return hot, gate

    @pl.loop(0, 16)
    def _(i):
        hot, gate = hot_of(lax.div(i, 2), lax.rem(i, 2), at.me)
        hot_a[pl.ds(pl.multiple_of(i * EXP, EXP), EXP), :] = hot
        gate_ref[i] = gate

    @pl.loop(0, 8)
    def _(i):
        src, mb = slot_of(at.core, lax.div(i, 2)), lax.rem(i, 2)
        row = pl.multiple_of(i * 2 * EXP, EXP)
        hot_b[pl.ds(row, EXP), :] = hot_of(src, mb, at.me)[0]
        hot_b[pl.ds(row + EXP, EXP), :] = hot_of(src, mb, at.partner)[0]
        ids_ref[i] = mg[src, 0, mb]

    def place_of(hot):
        before = dot(hot.astype(BF), tri[...])
        keep = jnp.logical_and(hot > 0.5, before < capacity)
        return jnp.where(keep, before, DROPPED)

    pos_ref[...] = place_of(hot_a[...]).reshape(pos_ref.shape)
    post_ref[...] = jnp.transpose(place_of(hot_b[...]))

    place = iota((capacity, tok), 0)
    per = EXP // 2

    def stored(b, kind, i):
        return pltpu.make_async_copy(stage.at[b], rows.at[kind, :, i], s_s.at[b])

    @pl.loop(0, 32)
    def _(t):
        u = lax.div(t, 8)
        first = lax.div((3 - u) * (2 - u) * (1 - u), 6)
        last = lax.div(u * (u - 1) * (u - 2), 6)
        sides = 1 - first - last

        @pl.when(t == 0)
        def _():
            for k in chunks[1:]:
                arrive(block(k, slot_of(at.other, at.chip)), by_c, k, at.dev_c)

        for k in chunks[1:]:

            @pl.when(t == 4 + 4 * k)
            def _():
                pass_on(k)

            @pl.when(t == 22 + 2 * k)
            def _():
                pass_on_corner(k)

        k0 = first * lax.div(t, 2) + sides * (lax.div(t, 4) - 2) + last * (lax.div(t, 2) - 12)
        kind, mb = lax.rem(k0, 2), lax.div(k0, 2)
        far = (first + last) * lax.rem(t, 2) + sides * lax.div(lax.rem(t, 4), 2)
        core = at.core + far * (1 - 2 * at.core)
        odd = lax.rem(t, 2)
        chip = at.chip + sides * ((1 - odd) * at.to_x + odd * at.to_y) + last * (at.to_x + at.to_y)
        src = slot_of(core, chip)
        i = src * 2 + mb
        b = lax.rem(t, 2)

        @pl.when(t >= 2)
        def _():
            stored(b, kind, i).wait()

        pos = pos_ref[i]
        for h in range(0, EXP, per):
            hot = jnp.concatenate([hot_bf(pos[e:e + 1, :] == place) for e in range(h, h + per)], axis=0)
            stage[b, h:h + per] = dot(hot, tg[kind, src, mb]).astype(BF).reshape(per, capacity, -1)
        stored(b, kind, i).start()

    for b in range(2):
        stored(b, 0, b).wait()
    for k in chunks:
        for hop in own_hops(k) + side_hops(k) + corner_hops(k):
            rcopy(*hop).wait_send()


def gather_rows(x_in, dy_out, meta, capacity):
    micro, tok, width = x_in.shape
    dma = pltpu.SemaphoreType.DMA
    table = jax.ShapeDtypeStruct((16, EXP, tok), F32)
    hots = pltpu.VMEM((LANES, tok), F32)
    return pl.pallas_call(
        functools.partial(gather_rows_kernel, capacity),
        out_shape=(jax.ShapeDtypeStruct((2, EXP, 16, capacity, width), BF), table, table, jax.ShapeDtypeStruct((tok, LANES), F32), jax.ShapeDtypeStruct((8, EXP, tok), F32)),
        in_specs=[ANY] * 3,
        out_specs=(ANY, VM, VM, VM, VM),
        scratch_shapes=[pltpu.VMEM((2, 8, micro, tok, width), BF), pltpu.VMEM((8,) + meta.shape, F32), hots, hots, pltpu.VMEM((tok, tok), BF), pltpu.VMEM((2, EXP, capacity, width), BF)] + [dma((5,))] * 19 + [dma((2,))],
        name='gather_rows',
        compiler_params=params(0),
        cost_estimate=cost(100, 80),
    )(x_in, dy_out, meta)


def expert_kernel(first, pos_ref, gate_ref, xr_ref, dyr_ref, wa_ref, dxr_ref, dg_ref, gw_ref, acc13, acc2):
    m = pl.program_id(1)
    e = pl.program_id(0) + first
    blocks, capacity, width = xr_ref.shape[2:]
    tok = pos_ref.shape[2]
    rows = blocks * capacity
    x = xr_ref[0, 0].reshape(rows, width)
    dy = dyr_ref[0, 0].reshape(rows, width)
    folds = [wa_ref[:, c // 2, 0, LANES * (c % 2):LANES * (c % 2) + LANES].reshape(width, LANES) for c in range(4)]
    w13 = jnp.concatenate(folds, axis=1)
    w2 = jnp.concatenate([wa_ref[z, 2, 0] for z in range(4)], axis=1)
    ff = w2.shape[0]
    place = iota((capacity, tok), 0)
    pos_rows = [pos_ref[m * blocks + b, pl.ds(e, 1), :] for b in range(blocks)]
    q = jnp.concatenate([jnp.sum(jnp.where(pos_rows[b] == place, gate_ref[m * blocks + b, pl.ds(e, 1), :], 0.0), axis=1, keepdims=True) for b in range(blocks)], axis=0)
    g = (q * dy.astype(F32)).astype(BF)
    h = dot(x, w13)
    dyw = lax.dot_general(dy, w2, NT, preferred_element_type=F32)
    da = lax.dot_general(g, w2, NT, preferred_element_type=F32)
    h1 = h[:, :ff]
    h3 = h[:, ff:]
    sig = jax.nn.sigmoid(h1)
    s = h1 * sig
    act = (s * h3).astype(BF)
    dg = jnp.sum(act.astype(F32) * dyw, axis=1, keepdims=True)
    dh3 = (da * s).astype(BF)
    dh1 = (da * h3 * sig * (1.0 + h1 * (1.0 - sig))).astype(BF)
    dh = jnp.concatenate([dh1, dh3], axis=1)
    dx = lax.dot_general(dh, w13, NT, preferred_element_type=F32).astype(BF)
    dxr_ref[0] = dx.reshape(blocks, capacity, width)
    for b in range(blocks):
        col = dg[b * capacity:(b + 1) * capacity]
        dg_ref[0, pl.ds(m * blocks + b, 1), :] = jnp.sum(jnp.where(pos_rows[b] == place, col, 0.0), axis=0, keepdims=True)
    g13 = lax.dot_general(x, dh, TN, preferred_element_type=F32)
    g2 = lax.dot_general(act, g, TN, preferred_element_type=F32)

    @pl.when(m == 0)
    def _():
        acc13[...] = g13
        acc2[...] = g2

    @pl.when(m > 0)
    def _():
        acc13[...] += g13
        acc2[...] += g2

    @pl.when(m == pl.num_programs(1) - 1)
    def _():
        for z in range(4):
            cols = slice(z * LANES, z * LANES + LANES)
            for c in range(4):
                gw_ref[z, c // 2, 0, LANES * (c % 2):LANES * (c % 2) + LANES] = acc13[cols, c * LANES:c * LANES + LANES]
            gw_ref[z, 2, 0] = acc2[:, cols]


def expert_pass(first, count, pos, gate, rows, w_all):
    blocks = 4
    pairs, capacity, width = rows.shape[2:]
    tok = pos.shape[2]

    def row_spec(kind):
        return pl.BlockSpec((1, 1, blocks, capacity, width), lambda e, m: (kind, e + first, m, 0, 0))

    weights = w_all.shape[3:]
    fold = (4, 3, 1) + weights
    return pl.pallas_call(
        functools.partial(expert_kernel, first),
        grid=(count, pairs // blocks),
        out_shape=(jax.ShapeDtypeStruct((count, pairs, capacity, width), BF), jax.ShapeDtypeStruct((count, pairs, tok), F32), jax.ShapeDtypeStruct((4, 3, count) + weights, F32)),
        in_specs=[VM, VM, row_spec(0), row_spec(1), pl.BlockSpec(fold, lambda e, m: (0, 0, e + first, 0, 0))],
        out_specs=(pl.BlockSpec((1, blocks, capacity, width), lambda e, m: (e, m, 0, 0)), pl.BlockSpec((1, pairs, tok), lambda e, m: (e, 0, 0)), pl.BlockSpec(fold, lambda e, m: (0, 0, e, 0, 0))),
        scratch_shapes=[pltpu.VMEM((width, width), F32), pltpu.VMEM((weights[0], width), F32)],
        name='expert_pass',
        compiler_params=params(),
        cost_estimate=cost(6 * count, 10 * count),
    )(pos, gate, rows, rows, w_all)


def reduce_kernel(groups, *refs):
    post_ref, ids_ref = refs[:2]
    rows, dgs = refs[2:2 + groups], refs[2 + groups:2 + 2 * groups]
    dx_ref, dgate_ref, hot, near, far, far_dg, q_ref, g_ref, in_x, in_y, last_x, last_y, g_in, g_last, s_h, s_f, r_f, s_d, r_d, s_x, r_x, s_y, r_y, s_2x, r_2x, s_2y, r_2y, s_g, r_g = refs[2 + 2 * groups:]
    at = Place()
    capacity, width = near.shape[2:]
    tok = post_ref.shape[0]
    half = tok // 2
    upper = pl.ds(0, half)
    lower = pl.ds(half, half)
    swap, swap_dg, hop_x, hop_y, hop_2x, hop_2y, hop_g = (s_f, r_f), (s_d, r_d), (s_x, r_x), (s_y, r_y), (s_2x, r_2x), (s_2y, r_2y), (s_g, r_g)
    firsts = [sum(ref.shape[0] for ref in rows[:n]) for n in range(groups)]

    def span(n):
        return pl.ds(firsts[n], rows[n].shape[0])

    def pair_of(t):
        p, mb = lax.div(t, 2), lax.rem(t, 2)
        return (at.chip + (1 - lax.div(p, 2)) * at.to_x + (1 - lax.rem(p, 2)) * at.to_y) * 2 + mb

    def loads(t):
        b = lax.rem(t, 2)
        return [pltpu.make_async_copy(rows[n].at[:, at.core * 8 + pair_of(t)], near.at[b, span(n)], s_h.at[b, n]) for n in range(groups)]

    def swaps(t):
        return [rcopy(rows[n].at[:, at.other * 8 + pair_of(t)], far.at[t, span(n)], swap, (n, t), at.dev_c) for n in range(groups)]

    def swaps_dg():
        return [rcopy(dgs[n].at[:, pl.ds(pl.multiple_of(at.other * 8, 8), 8)], far_dg.at[span(n)], swap_dg, n, at.dev_c) for n in range(groups)]

    def send(src, dst, sems, i, dev):
        rcopy(src, dst, sems, i, dev).start()

    def sent(src, dst, sems, i, dev):
        rcopy(src, dst, sems, i, dev).wait_send()

    def first_hops(p, mb):
        hops = []
        if p < 2:
            hops.append((q_ref.at[p, mb, upper], in_x.at[mb, 1 - p], hop_x, 2 * mb + 1 - p, at.dev_x))
        if p % 2 == 0:
            hops.append((q_ref.at[p, mb, lower], in_y.at[mb, 1 - p // 2], hop_y, 2 * mb + 1 - p // 2, at.dev_y))
        return hops

    def gate_hop(p):
        return (g_ref.at[p], g_in.at[1 - p], hop_g, 1 - p, at.dev_x)

    for copy in loads(0):
        copy.start()
    at.greet()

    @pl.loop(0, 8)
    def _(t):
        for copy in swaps(t):
            copy.start()

        @pl.when(t == 0)
        def _():
            for copy in swaps_dg():
                copy.start()

    lane = iota((tok, LANES), 1)
    tiles = 2 * EXP * capacity // LANES

    @pl.loop(0, 8)
    def _(t):
        p, mb = lax.div(t, 2), lax.rem(t, 2)
        i = pair_of(t)

        @pl.when(t < 7)
        def _():
            for copy in loads(t + 1):
                copy.start()

        post = pltpu.roll(post_ref[...], lax.rem(LANES - i * 2 * EXP, LANES), 1)
        for k in range(tiles):
            col = k * LANES
            lo = col // capacity
            sel = post[:, lo:lo + 1] == lane + (col - lo * capacity)
            for e in range(lo + 1, (col + LANES - 1) // capacity + 1):
                sel = jnp.logical_or(sel, post[:, e:e + 1] == lane + (col - e * capacity))
            hot[:, col:col + LANES] = hot_bf(sel)
        for copy in loads(t):
            copy.wait()
        for copy in swaps(t):
            copy.wait_recv()

        @pl.when(t == 0)
        def _():
            for copy in swaps_dg():
                copy.wait_recv()

        rows_near = near[mb].reshape(EXP * capacity, width)
        rows_far = far[t].reshape(EXP * capacity, width)
        q_ref[p, mb] = dot(hot[...], jnp.concatenate([rows_near, rows_far], axis=0))
        ids = ids_ref[i]
        total = jnp.zeros(ids.shape, F32)
        for n in range(groups):
            for c in range(rows[n].shape[0]):
                e = firsts[n] + c
                mine = dgs[n][c, pl.ds(at.core * 8 + i, 1), :]
                total = jnp.where(ids == (at.me * EXP + e).astype(F32), mine, total)
                total = jnp.where(ids == (at.partner * EXP + e).astype(F32), far_dg[e, pl.ds(i, 1), :], total)
        g_ref[p, mb] = total
        for c in range(3):

            @pl.when(p == c)
            def _():
                for hop in first_hops(c, mb):
                    send(*hop)

        for c in range(2):

            @pl.when(t == 2 * c + 1)
            def _():
                send(*gate_hop(c))

    arrive(g_in.at[1], hop_g, 1, at.dev_x)
    g_in[1] += g_ref[2]
    gate_last = (g_in.at[1], g_last, hop_g, 2, at.dev_y)
    send(*gate_last)

    def last_hops(mb):
        return ((in_x.at[mb, 1], last_y.at[mb], hop_2y, mb, at.dev_y), (in_y.at[mb, 1], last_x.at[mb], hop_2x, mb, at.dev_x))

    for mb in range(2):
        hops = last_hops(mb)
        arrive(in_x.at[mb, 1], hop_x, 2 * mb + 1, at.dev_x)
        in_x[mb, 1] += q_ref[2, mb, upper]
        send(*hops[0])
        arrive(in_y.at[mb, 1], hop_y, 2 * mb + 1, at.dev_y)
        in_y[mb, 1] += q_ref[1, mb, lower]
        send(*hops[1])
    arrive(g_in.at[0], hop_g, 0, at.dev_x)
    arrive(g_last, hop_g, 2, at.dev_y)
    dgate_ref[...] = g_ref[3] + g_in[0] + g_last[...]
    for mb in range(2):
        arrive(in_x.at[mb, 0], hop_x, 2 * mb, at.dev_x)
        arrive(in_y.at[mb, 0], hop_y, 2 * mb, at.dev_y)
        q_ref[3, mb, upper] += in_x[mb, 0]
        q_ref[3, mb, lower] += in_y[mb, 0]
    for mb in range(2):
        arrive(last_y.at[mb], hop_2y, mb, at.dev_y)
        dx_ref[mb, upper] = (q_ref[3, mb, upper] + last_y[mb]).astype(BF)
        arrive(last_x.at[mb], hop_2x, mb, at.dev_x)
        dx_ref[mb, lower] = (q_ref[3, mb, lower] + last_x[mb]).astype(BF)
    for mb in range(2):
        sent(*gate_hop(mb))
        for c in range(3):
            for hop in first_hops(c, mb):
                sent(*hop)
        for hop in last_hops(mb):
            sent(*hop)
    sent(*gate_last)
    for copy in swaps_dg():
        copy.wait_send()

    @pl.loop(0, 8)
    def _(t):
        for copy in swaps(t):
            copy.wait_send()


def reduce_chips(post, ids, rows, dgs):
    groups = len(rows)
    capacity, width = rows[0].shape[2:]
    tok = post.shape[0]
    top_k = ids.shape[1]
    half = tok // 2
    dma = pltpu.SemaphoreType.DMA
    vm = pltpu.VMEM
    return pl.pallas_call(
        functools.partial(reduce_kernel, groups),
        out_shape=(jax.ShapeDtypeStruct((2, tok, width), BF), jax.ShapeDtypeStruct((2, top_k, tok), F32)),
        in_specs=[VM, VM] + [ANY] * groups + [VM] * groups,
        out_specs=(VM, VM),
        scratch_shapes=[vm((tok, 2 * EXP * capacity), BF), vm((2, EXP, capacity, width), BF), vm((8, EXP, capacity, width), BF), vm((EXP, 8, tok), F32), vm((4, 2, tok, width), F32), vm((4, 2, top_k, tok), F32)]
        + [vm((2, 2, half, width), F32)] * 2 + [vm((2, half, width), F32)] * 2 + [vm((2, 2, top_k, tok), F32), vm((2, top_k, tok), F32), dma((2, groups))]
        + [dma((groups, 8))] * 2 + [dma((groups,))] * 2 + [dma((4,))] * 4 + [dma((2,))] * 4 + [dma((3,))] * 2,
        name='reduce_chips',
        compiler_params=params(2),
        cost_estimate=cost(100, 40),
    )(post, ids, *rows, *dgs)


def solution(mesh):
    ep_size = mesh.shape['ep']
    tok_spec = P(None, ('fsdp', 'ep'), None)
    spec_edf = P('ep', 'fsdp', None)
    spec_efd = P('ep', None, 'fsdp')

    def fold(w):
        return jnp.concatenate([w[:, :, :LANES], w[:, :, LANES:]], axis=1)

    def unfold(g):
        return jnp.concatenate([g[:, :LANES], g[:, LANES:]], axis=2)

    def local_step(x_in, dy_out, expert_idx, gate_prob, w_one, w_two, w_three):
        micro, tok, width = x_in.shape
        top_k = expert_idx.shape[2]
        local_experts = w_one.shape[0]
        capacity = capacity_of(tok, top_k, local_experts * ep_size)
        w_mine = jnp.concatenate([fold(w_one), fold(w_three), w_two], axis=0)
        w_all = lax.all_gather(w_mine, 'fsdp', axis=0, tiled=False)
        w_all = w_all.reshape((w_all.shape[0], 3, local_experts) + w_two.shape[1:])
        meta = jnp.stack([jnp.transpose(expert_idx, (0, 2, 1)).astype(F32), jnp.transpose(gate_prob, (0, 2, 1))])
        rows, pos, gate, post, ids = gather_rows(x_in, dy_out, meta, capacity)
        dx_rows, dgs, grads = [], [], []
        for count in GROUPS:
            first = sum(r.shape[0] for r in dx_rows)
            r, d, g = expert_pass(first, count, pos, gate, rows, w_all)
            dx_rows.append(r)
            dgs.append(d)
            grads.append(lax.psum_scatter(g, 'fsdp', scatter_dimension=0, tiled=False))
        dx, dgate = reduce_chips(post, ids, dx_rows, dgs)
        grad = jnp.concatenate(grads, axis=1)
        return dx, jnp.transpose(dgate, (0, 2, 1)), unfold(grad[0]), grad[2], unfold(grad[1])

    return jax.shard_map(local_step, mesh=mesh, in_specs=(tok_spec, tok_spec, tok_spec, tok_spec, spec_edf, spec_efd, spec_edf), out_specs=(tok_spec, tok_spec, spec_edf, spec_efd, spec_edf), check_vma=False)
```

```python
import functools

import jax
import jax.numpy as jnp
from jax import lax
from jax.experimental import pallas as pl
from jax.experimental.pallas import tpu as pltpu
from jax.sharding import PartitionSpec as P

MESH = pl.DeviceIdType.MESH
BF = jnp.bfloat16
F32 = jnp.float32
ANY = pl.BlockSpec(memory_space=pl.ANY)
VM = pl.BlockSpec(memory_space=pltpu.VMEM)
VLIM = 62 * 1024 * 1024
GROUPS = (1, 3, 4)
DROPPED = -4096.0
LANES = 128
EXP = 8
NT = (((1,), (1,)), ((), ()))
TN = (((0,), (0,)), ((), ()))


def params(collective_id=None):
    if collective_id is None:
        return pltpu.CompilerParams(vmem_limit_bytes=VLIM)
    return pltpu.CompilerParams(collective_id=collective_id, has_side_effects=True, vmem_limit_bytes=VLIM)


def cost(gflop, mbytes):
    return pl.CostEstimate(flops=gflop * 10**9, bytes_accessed=mbytes * 10**6, transcendentals=0)


def capacity_of(tok_rows, top_k, experts):
    return 8 * ((5 * tok_rows * top_k + 32 * experts - 1) // (32 * experts))


def dot(a, b):
    return jnp.dot(a, b, preferred_element_type=F32)


def hot_bf(sel):
    return jnp.where(sel, 1.0, 0.0).astype(BF)


def iota(shape, dim):
    return lax.broadcasted_iota(jnp.int32, shape, dim).astype(F32)


class Place:
    def __init__(self):
        me = lax.axis_index('ep')
        z = lax.axis_index('fsdp')
        self.me = me
        self.core = lax.rem(me, 2)
        self.other = 1 - self.core
        self.partner = me + 1 - 2 * self.core
        self.chip = lax.div(me, 2)
        self.to_x = 1 - 2 * lax.rem(self.chip, 2)
        self.to_y = 2 - 4 * lax.div(self.chip, 2)
        self.chip_x = self.chip + self.to_x
        self.chip_y = self.chip + self.to_y
        self.chip_d = self.chip_x + self.to_y
        self.dev_x = (z, 2 * self.chip_x + self.core)
        self.dev_y = (z, 2 * self.chip_y + self.core)
        self.dev_d = (z, 2 * self.chip_d + self.core)
        self.dev_c = (z, self.partner)

    def greet(self, *devices):
        barrier = pltpu.get_barrier_semaphore()
        for dev in devices:
            pl.semaphore_signal(barrier, inc=1, device_id=dev, device_id_type=MESH)
        pl.semaphore_wait(barrier, len(devices))


def rcopy(src, dst, sems, i, dev):
    return pltpu.make_async_remote_copy(src_ref=src, dst_ref=dst, send_sem=sems[0].at[i], recv_sem=sems[1].at[i], device_id=dev, device_id_type=MESH)


def arrive(ref, sems, i, dev):
    rcopy(ref, ref, sems, i, dev).wait_recv()


def gather_rows_kernel(capacity, x_ref, dy_ref, meta_ref, rows, pos_ref, gate_ref, post_ref, ids_ref, tg, mg, hot_a, hot_b, tri, stage, s_x, r_x, s_y, r_y, s_c, r_c, s_ax, r_ax, s_ay, r_ay, s_fx, r_fx, s_fy, r_fy, s_fa, r_fa, s_fb, r_fb, s_l, s_s):
    at = Place()
    tok = x_ref.shape[1]
    half = tok // 2
    by_x, by_y, by_c, relay_x, relay_y = (s_x, r_x), (s_y, r_y), (s_c, r_c), (s_ax, r_ax), (s_ay, r_ay)
    fwd_x, fwd_y, fwd_a, fwd_b = (s_fx, r_fx), (s_fy, r_fy), (s_fa, r_fa), (s_fb, r_fb)
    chunks = range(5)

    def slot_of(core, chip):
        return core * 4 + chip

    def own(k):
        if k == 0:
            return meta_ref
        return (dy_ref, x_ref)[k % 2].at[(k - 1) // 2]

    def block(k, slot):
        if k == 0:
            return mg.at[slot]
        return tg.at[(k - 1) % 2, slot, (k - 1) // 2]

    def part(k, slot, h):
        return block(k, slot).at[pl.ds(h * half, half)]

    slot = slot_of(at.core, at.chip)
    slot_x = slot_of(at.core, at.chip_x)
    slot_y = slot_of(at.core, at.chip_y)
    slot_d = slot_of(at.core, at.chip_d)

    def side_hops(k):
        return (
            (part(k, slot_x, 0), part(k, slot_x, 0), relay_y, k, at.dev_y),
            (block(k, slot_x), block(k, slot_x), fwd_x, k, at.dev_c),
            (part(k, slot_y, 1), part(k, slot_y, 1), relay_x, k, at.dev_x),
            (block(k, slot_y), block(k, slot_y), fwd_y, k, at.dev_c),
        )

    def corner_hops(k):
        return ((part(k, slot_d, 0), part(k, slot_d, 0), fwd_a, k, at.dev_c), (part(k, slot_d, 1), part(k, slot_d, 1), fwd_b, k, at.dev_c))

    def own_hops(k):
        return tuple((own(k), block(k, slot), sems, k, dev) for sems, dev in ((by_c, at.dev_c), (by_x, at.dev_x), (by_y, at.dev_y)))

    def meta_hops():
        return tuple((meta_ref, mg.at[slot], sems, 0, dev) for sems, dev in ((relay_x, at.dev_d), (by_x, at.dev_x), (by_y, at.dev_y), (by_c, at.dev_c)))

    def meta_shares():
        return tuple((mg.at[src], mg.at[src], sems, 0, at.dev_c) for src, sems in ((slot_x, fwd_x), (slot_y, fwd_y), (slot_d, fwd_a)))

    def send(hops):
        for hop in hops:
            rcopy(*hop).start()

    def pass_on(k):
        hops = side_hops(k)
        arrive(block(k, slot_x), by_x, k, at.dev_x)
        send(hops[:2])
        arrive(block(k, slot_y), by_y, k, at.dev_y)
        send(hops[2:])
        arrive(block(k, slot_of(at.other, at.chip_x)), fwd_x, k, at.dev_c)
        arrive(block(k, slot_of(at.other, at.chip_y)), fwd_y, k, at.dev_c)

    def pass_on_corner(k):
        hops = corner_hops(k)
        far = slot_of(at.other, at.chip_d)
        arrive(part(k, slot_d, 0), relay_y, k, at.dev_y)
        send(hops[:1])
        arrive(part(k, slot_d, 1), relay_x, k, at.dev_x)
        send(hops[1:])
        arrive(part(k, far, 0), fwd_a, k, at.dev_c)
        arrive(part(k, far, 1), fwd_b, k, at.dev_c)

    local = [pltpu.make_async_copy(own(k), block(k, slot), s_l.at[k]) for k in chunks]
    for copy in local:
        copy.start()
    at.greet(at.dev_x, at.dev_y, at.dev_d, at.dev_c)
    send(meta_hops())
    for k in chunks[1:]:
        send(own_hops(k))

    tri[...] = hot_bf(iota((tok, tok), 0) < iota((tok, tok), 1))
    for copy in local:
        copy.wait()
    arrive(mg.at[slot_of(at.other, at.chip)], by_c, 0, at.dev_c)
    shared = meta_shares()
    for n, (src, sems, dev) in enumerate(((slot_x, by_x, at.dev_x), (slot_y, by_y, at.dev_y), (slot_d, relay_x, at.dev_d))):
        arrive(mg.at[src], sems, 0, dev)
        send(shared[n:n + 1])
    for chip, sems in ((at.chip_x, fwd_x), (at.chip_y, fwd_y), (at.chip_d, fwd_a)):
        arrive(mg.at[slot_of(at.other, chip)], sems, 0, at.dev_c)
    sub = iota((EXP, tok), 0)

    def hot_of(src, mb, device):
        ids = mg[src, 0, mb]
        vals = mg[src, 1, mb]
        want = sub + (device * EXP).astype(F32)
        hot = jnp.zeros((EXP, tok), F32)
        gate = hot
        for j in range(ids.shape[0]):
            sel = ids[j:j + 1, :] == want
            hot = jnp.where(sel, 1.0, hot)
            gate = jnp.where(sel, vals[j:j + 1, :], gate)
        return hot, gate

    @pl.loop(0, 16)
    def _(i):
        hot, gate = hot_of(lax.div(i, 2), lax.rem(i, 2), at.me)
        hot_a[pl.ds(pl.multiple_of(i * EXP, EXP), EXP), :] = hot
        gate_ref[i] = gate

    @pl.loop(0, 8)
    def _(i):
        src, mb = slot_of(at.core, lax.div(i, 2)), lax.rem(i, 2)
        row = pl.multiple_of(i * 2 * EXP, EXP)
        hot_b[pl.ds(row, EXP), :] = hot_of(src, mb, at.me)[0]
        hot_b[pl.ds(row + EXP, EXP), :] = hot_of(src, mb, at.partner)[0]
        ids_ref[i] = mg[src, 0, mb]

    def place_of(hot):
        before = dot(hot.astype(BF), tri[...])
        keep = jnp.logical_and(hot > 0.5, before < capacity)
        return jnp.where(keep, before, DROPPED)

    pos_ref[...] = place_of(hot_a[...]).reshape(pos_ref.shape)
    post_ref[...] = jnp.transpose(place_of(hot_b[...]))

    place = iota((capacity, tok), 0)
    per = EXP // 2

    def stored(b, kind, i):
        return pltpu.make_async_copy(stage.at[b], rows.at[kind, :, i], s_s.at[b])

    @pl.loop(0, 32)
    def _(t):
        u = lax.div(t, 8)
        first = lax.div((3 - u) * (2 - u) * (1 - u), 6)
        last = lax.div(u * (u - 1) * (u - 2), 6)
        sides = 1 - first - last

        @pl.when(t == 0)
        def _():
            for k in chunks[1:]:
                arrive(block(k, slot_of(at.other, at.chip)), by_c, k, at.dev_c)

        for k in chunks[1:]:

            @pl.when(t == 4 + 4 * k)
            def _():
                pass_on(k)

            @pl.when(t == 22 + 2 * k)
            def _():
                pass_on_corner(k)

        k0 = first * lax.div(t, 2) + sides * (lax.div(t, 4) - 2) + last * (lax.div(t, 2) - 12)
        kind, mb = lax.rem(k0, 2), lax.div(k0, 2)
        far = (first + last) * lax.rem(t, 2) + sides * lax.div(lax.rem(t, 4), 2)
        core = at.core + far * (1 - 2 * at.core)
        odd = lax.rem(t, 2)
        chip = at.chip + sides * ((1 - odd) * at.to_x + odd * at.to_y) + last * (at.to_x + at.to_y)
        src = slot_of(core, chip)
        i = src * 2 + mb
        b = lax.rem(t, 2)

        @pl.when(t >= 2)
        def _():
            stored(b, kind, i).wait()

        pos = pos_ref[i]
        for h in range(0, EXP, per):
            hot = jnp.concatenate([hot_bf(pos[e:e + 1, :] == place) for e in range(h, h + per)], axis=0)
            stage[b, h:h + per] = dot(hot, tg[kind, src, mb]).astype(BF).reshape(per, capacity, -1)
        stored(b, kind, i).start()

    for b in range(2):
        stored(b, 0, b).wait()
    for hop in meta_hops() + meta_shares():
        rcopy(*hop).wait_send()
    for k in chunks[1:]:
        for hop in own_hops(k) + side_hops(k) + corner_hops(k):
            rcopy(*hop).wait_send()


def gather_rows(x_in, dy_out, meta, capacity):
    micro, tok, width = x_in.shape
    dma = pltpu.SemaphoreType.DMA
    table = jax.ShapeDtypeStruct((16, EXP, tok), F32)
    hots = pltpu.VMEM((LANES, tok), F32)
    return pl.pallas_call(
        functools.partial(gather_rows_kernel, capacity),
        out_shape=(jax.ShapeDtypeStruct((2, EXP, 16, capacity, width), BF), table, table, jax.ShapeDtypeStruct((tok, LANES), F32), jax.ShapeDtypeStruct((8, EXP, tok), F32)),
        in_specs=[ANY] * 3,
        out_specs=(ANY, VM, VM, VM, VM),
        scratch_shapes=[pltpu.VMEM((2, 8, micro, tok, width), BF), pltpu.VMEM((8,) + meta.shape, F32), hots, hots, pltpu.VMEM((tok, tok), BF), pltpu.VMEM((2, EXP, capacity, width), BF)] + [dma((5,))] * 19 + [dma((2,))],
        name='gather_rows',
        compiler_params=params(0),
        cost_estimate=cost(100, 80),
    )(x_in, dy_out, meta)


def expert_kernel(first, pos_ref, gate_ref, xr_ref, dyr_ref, wa_ref, dxr_ref, dg_ref, gw_ref, acc13, acc2):
    m = pl.program_id(1)
    e = pl.program_id(0) + first
    blocks, capacity, width = xr_ref.shape[2:]
    tok = pos_ref.shape[2]
    rows = blocks * capacity
    x = xr_ref[0, 0].reshape(rows, width)
    dy = dyr_ref[0, 0].reshape(rows, width)
    folds = [wa_ref[:, c // 2, 0, LANES * (c % 2):LANES * (c % 2) + LANES].reshape(width, LANES) for c in range(4)]
    w13 = jnp.concatenate(folds, axis=1)
    w2 = jnp.concatenate([wa_ref[z, 2, 0] for z in range(4)], axis=1)
    ff = w2.shape[0]
    place = iota((capacity, tok), 0)
    pos_rows = [pos_ref[m * blocks + b, pl.ds(e, 1), :] for b in range(blocks)]
    q = jnp.concatenate([jnp.sum(jnp.where(pos_rows[b] == place, gate_ref[m * blocks + b, pl.ds(e, 1), :], 0.0), axis=1, keepdims=True) for b in range(blocks)], axis=0)
    g = (q * dy.astype(F32)).astype(BF)
    h = dot(x, w13)
    dyw = lax.dot_general(dy, w2, NT, preferred_element_type=F32)
    da = lax.dot_general(g, w2, NT, preferred_element_type=F32)
    h1 = h[:, :ff]
    h3 = h[:, ff:]
    sig = jax.nn.sigmoid(h1)
    s = h1 * sig
    act = (s * h3).astype(BF)
    dg = jnp.sum(act.astype(F32) * dyw, axis=1, keepdims=True)
    dh3 = (da * s).astype(BF)
    dh1 = (da * h3 * sig * (1.0 + h1 * (1.0 - sig))).astype(BF)
    dh = jnp.concatenate([dh1, dh3], axis=1)
    dx = lax.dot_general(dh, w13, NT, preferred_element_type=F32).astype(BF)
    dxr_ref[0] = dx.reshape(blocks, capacity, width)
    for b in range(blocks):
        col = dg[b * capacity:(b + 1) * capacity]
        dg_ref[0, pl.ds(m * blocks + b, 1), :] = jnp.sum(jnp.where(pos_rows[b] == place, col, 0.0), axis=0, keepdims=True)
    g13 = lax.dot_general(x, dh, TN, preferred_element_type=F32)
    g2 = lax.dot_general(act, g, TN, preferred_element_type=F32)

    @pl.when(m == 0)
    def _():
        acc13[...] = g13
        acc2[...] = g2

    @pl.when(m > 0)
    def _():
        acc13[...] += g13
        acc2[...] += g2

    @pl.when(m == pl.num_programs(1) - 1)
    def _():
        for z in range(4):
            cols = slice(z * LANES, z * LANES + LANES)
            for c in range(4):
                gw_ref[z, c // 2, 0, LANES * (c % 2):LANES * (c % 2) + LANES] = acc13[cols, c * LANES:c * LANES + LANES]
            gw_ref[z, 2, 0] = acc2[:, cols]


def expert_pass(first, count, pos, gate, rows, w_all):
    blocks = 8
    pairs, capacity, width = rows.shape[2:]
    tok = pos.shape[2]

    def row_spec(kind):
        return pl.BlockSpec((1, 1, blocks, capacity, width), lambda e, m: (kind, e + first, m, 0, 0))

    weights = w_all.shape[3:]
    fold = (4, 3, 1) + weights
    return pl.pallas_call(
        functools.partial(expert_kernel, first),
        grid=(count, pairs // blocks),
        out_shape=(jax.ShapeDtypeStruct((count, pairs, capacity, width), BF), jax.ShapeDtypeStruct((count, pairs, tok), F32), jax.ShapeDtypeStruct((4, 3, count) + weights, F32)),
        in_specs=[VM, VM, row_spec(0), row_spec(1), pl.BlockSpec(fold, lambda e, m: (0, 0, e + first, 0, 0))],
        out_specs=(pl.BlockSpec((1, blocks, capacity, width), lambda e, m: (e, m, 0, 0)), pl.BlockSpec((1, pairs, tok), lambda e, m: (e, 0, 0)), pl.BlockSpec(fold, lambda e, m: (0, 0, e, 0, 0))),
        scratch_shapes=[pltpu.VMEM((width, width), F32), pltpu.VMEM((weights[0], width), F32)],
        name='expert_pass',
        compiler_params=params(),
        cost_estimate=cost(6 * count, 10 * count),
    )(pos, gate, rows, rows, w_all)


def reduce_kernel(groups, *refs):
    post_ref, ids_ref = refs[:2]
    rows, dgs = refs[2:2 + groups], refs[2 + groups:2 + 2 * groups]
    dx_ref, dgate_ref, hot, near, far, far_dg, q_ref, g_ref, in_x, in_y, last_x, last_y, g_in, g_last, s_h, s_f, r_f, s_d, r_d, s_x, r_x, s_y, r_y, s_2x, r_2x, s_2y, r_2y, s_g, r_g = refs[2 + 2 * groups:]
    at = Place()
    capacity, width = near.shape[2:]
    tok = post_ref.shape[0]
    half = tok // 2
    upper = pl.ds(0, half)
    lower = pl.ds(half, half)
    swap, swap_dg, hop_x, hop_y, hop_2x, hop_2y, hop_g = (s_f, r_f), (s_d, r_d), (s_x, r_x), (s_y, r_y), (s_2x, r_2x), (s_2y, r_2y), (s_g, r_g)
    firsts = [sum(ref.shape[0] for ref in rows[:n]) for n in range(groups)]

    def span(n):
        return pl.ds(firsts[n], rows[n].shape[0])

    def pair_of(t):
        p, mb = lax.div(t, 2), lax.rem(t, 2)
        return (at.chip + (1 - lax.div(p, 2)) * at.to_x + (1 - lax.rem(p, 2)) * at.to_y) * 2 + mb

    def loads(t):
        b = lax.rem(t, 2)
        return [pltpu.make_async_copy(rows[n].at[:, at.core * 8 + pair_of(t)], near.at[b, span(n)], s_h.at[b, n]) for n in range(groups)]

    def swaps(t):
        return [rcopy(rows[n].at[:, at.other * 8 + pair_of(t)], far.at[t, span(n)], swap, (n, t), at.dev_c) for n in range(groups)]

    def swaps_dg():
        return [rcopy(dgs[n].at[:, pl.ds(pl.multiple_of(at.other * 8, 8), 8)], far_dg.at[span(n)], swap_dg, n, at.dev_c) for n in range(groups)]

    def send(src, dst, sems, i, dev):
        rcopy(src, dst, sems, i, dev).start()

    def sent(src, dst, sems, i, dev):
        rcopy(src, dst, sems, i, dev).wait_send()

    def first_hops(p, mb):
        hops = []
        if p < 2:
            hops.append((q_ref.at[p, mb, upper], in_x.at[mb, 1 - p], hop_x, 2 * mb + 1 - p, at.dev_x))
        if p % 2 == 0:
            hops.append((q_ref.at[p, mb, lower], in_y.at[mb, 1 - p // 2], hop_y, 2 * mb + 1 - p // 2, at.dev_y))
        return hops

    def gate_hop(p):
        return (g_ref.at[p], g_in.at[1 - p], hop_g, 1 - p, at.dev_x)

    for copy in loads(0):
        copy.start()
    at.greet(at.dev_x, at.dev_y, at.dev_c)

    @pl.loop(0, 8)
    def _(t):
        for copy in swaps(t):
            copy.start()

        @pl.when(t == 0)
        def _():
            for copy in swaps_dg():
                copy.start()

    lane = iota((tok, LANES), 1)
    tiles = 2 * EXP * capacity // LANES

    @pl.loop(0, 8)
    def _(t):
        p, mb = lax.div(t, 2), lax.rem(t, 2)
        i = pair_of(t)

        @pl.when(t < 7)
        def _():
            for copy in loads(t + 1):
                copy.start()

        post = pltpu.roll(post_ref[...], lax.rem(LANES - i * 2 * EXP, LANES), 1)
        for k in range(tiles):
            col = k * LANES
            lo = col // capacity
            sel = post[:, lo:lo + 1] == lane + (col - lo * capacity)
            for e in range(lo + 1, (col + LANES - 1) // capacity + 1):
                sel = jnp.logical_or(sel, post[:, e:e + 1] == lane + (col - e * capacity))
            hot[:, col:col + LANES] = hot_bf(sel)
        for copy in loads(t):
            copy.wait()
        for copy in swaps(t):
            copy.wait_recv()

        @pl.when(t == 0)
        def _():
            for copy in swaps_dg():
                copy.wait_recv()

        rows_near = near[mb].reshape(EXP * capacity, width)
        rows_far = far[t].reshape(EXP * capacity, width)
        q_ref[p, mb] = dot(hot[...], jnp.concatenate([rows_near, rows_far], axis=0))
        ids = ids_ref[i]
        total = jnp.zeros(ids.shape, F32)
        for n in range(groups):
            for c in range(rows[n].shape[0]):
                e = firsts[n] + c
                mine = dgs[n][c, pl.ds(at.core * 8 + i, 1), :]
                total = jnp.where(ids == (at.me * EXP + e).astype(F32), mine, total)
                total = jnp.where(ids == (at.partner * EXP + e).astype(F32), far_dg[e, pl.ds(i, 1), :], total)
        g_ref[p, mb] = total
        for c in range(3):

            @pl.when(p == c)
            def _():
                for hop in first_hops(c, mb):
                    send(*hop)

        for c in range(2):

            @pl.when(t == 2 * c + 1)
            def _():
                send(*gate_hop(c))

    arrive(g_in.at[1], hop_g, 1, at.dev_x)
    g_in[1] += g_ref[2]
    gate_last = (g_in.at[1], g_last, hop_g, 2, at.dev_y)
    send(*gate_last)

    def last_hops(mb):
        return ((in_x.at[mb, 1], last_y.at[mb], hop_2y, mb, at.dev_y), (in_y.at[mb, 1], last_x.at[mb], hop_2x, mb, at.dev_x))

    for mb in range(2):
        hops = last_hops(mb)
        arrive(in_x.at[mb, 1], hop_x, 2 * mb + 1, at.dev_x)
        in_x[mb, 1] += q_ref[2, mb, upper]
        send(*hops[0])
        arrive(in_y.at[mb, 1], hop_y, 2 * mb + 1, at.dev_y)
        in_y[mb, 1] += q_ref[1, mb, lower]
        send(*hops[1])
    arrive(g_in.at[0], hop_g, 0, at.dev_x)
    arrive(g_last, hop_g, 2, at.dev_y)
    dgate_ref[...] = g_ref[3] + g_in[0] + g_last[...]
    for mb in range(2):
        arrive(in_x.at[mb, 0], hop_x, 2 * mb, at.dev_x)
        arrive(in_y.at[mb, 0], hop_y, 2 * mb, at.dev_y)
        q_ref[3, mb, upper] += in_x[mb, 0]
        q_ref[3, mb, lower] += in_y[mb, 0]
    for mb in range(2):
        arrive(last_y.at[mb], hop_2y, mb, at.dev_y)
        dx_ref[mb, upper] = (q_ref[3, mb, upper] + last_y[mb]).astype(BF)
        arrive(last_x.at[mb], hop_2x, mb, at.dev_x)
        dx_ref[mb, lower] = (q_ref[3, mb, lower] + last_x[mb]).astype(BF)
    for mb in range(2):
        sent(*gate_hop(mb))
        for c in range(3):
            for hop in first_hops(c, mb):
                sent(*hop)
        for hop in last_hops(mb):
            sent(*hop)
    sent(*gate_last)
    for copy in swaps_dg():
        copy.wait_send()

    @pl.loop(0, 8)
    def _(t):
        for copy in swaps(t):
            copy.wait_send()


def reduce_chips(post, ids, rows, dgs):
    groups = len(rows)
    capacity, width = rows[0].shape[2:]
    tok = post.shape[0]
    top_k = ids.shape[1]
    half = tok // 2
    dma = pltpu.SemaphoreType.DMA
    vm = pltpu.VMEM
    return pl.pallas_call(
        functools.partial(reduce_kernel, groups),
        out_shape=(jax.ShapeDtypeStruct((2, tok, width), BF), jax.ShapeDtypeStruct((2, top_k, tok), F32)),
        in_specs=[VM, VM] + [ANY] * groups + [VM] * groups,
        out_specs=(VM, VM),
        scratch_shapes=[vm((tok, 2 * EXP * capacity), BF), vm((2, EXP, capacity, width), BF), vm((8, EXP, capacity, width), BF), vm((EXP, 8, tok), F32), vm((4, 2, tok, width), F32), vm((4, 2, top_k, tok), F32)]
        + [vm((2, 2, half, width), F32)] * 2 + [vm((2, half, width), F32)] * 2 + [vm((2, 2, top_k, tok), F32), vm((2, top_k, tok), F32), dma((2, groups))]
        + [dma((groups, 8))] * 2 + [dma((groups,))] * 2 + [dma((4,))] * 4 + [dma((2,))] * 4 + [dma((3,))] * 2,
        name='reduce_chips',
        compiler_params=params(2),
        cost_estimate=cost(100, 40),
    )(post, ids, *rows, *dgs)


def solution(mesh):
    ep_size = mesh.shape['ep']
    tok_spec = P(None, ('fsdp', 'ep'), None)
    spec_edf = P('ep', 'fsdp', None)
    spec_efd = P('ep', None, 'fsdp')

    def fold(w):
        return jnp.concatenate([w[:, :, :LANES], w[:, :, LANES:]], axis=1)

    def unfold(g):
        return jnp.concatenate([g[:, :LANES], g[:, LANES:]], axis=2)

    def local_step(x_in, dy_out, expert_idx, gate_prob, w_one, w_two, w_three):
        micro, tok, width = x_in.shape
        top_k = expert_idx.shape[2]
        local_experts = w_one.shape[0]
        capacity = capacity_of(tok, top_k, local_experts * ep_size)
        w_mine = jnp.concatenate([fold(w_one), fold(w_three), w_two], axis=0)
        w_all = lax.all_gather(w_mine, 'fsdp', axis=0, tiled=False)
        w_all = w_all.reshape((w_all.shape[0], 3, local_experts) + w_two.shape[1:])
        meta = jnp.stack([jnp.transpose(expert_idx, (0, 2, 1)).astype(F32), jnp.transpose(gate_prob, (0, 2, 1))])
        rows, pos, gate, post, ids = gather_rows(x_in, dy_out, meta, capacity)
        dx_rows, dgs, grads = [], [], []
        for count in GROUPS:
            first = sum(r.shape[0] for r in dx_rows)
            r, d, g = expert_pass(first, count, pos, gate, rows, w_all)
            dx_rows.append(r)
            dgs.append(d)
            grads.append(lax.psum_scatter(g, 'fsdp', scatter_dimension=0, tiled=False))
        dx, dgate = reduce_chips(post, ids, dx_rows, dgs)
        grad = jnp.concatenate(grads, axis=1)
        return dx, jnp.transpose(dgate, (0, 2, 1)), unfold(grad[0]), grad[2], unfold(grad[1])

    return jax.shard_map(local_step, mesh=mesh, in_specs=(tok_spec, tok_spec, tok_spec, tok_spec, spec_edf, spec_efd, spec_edf), out_specs=(tok_spec, tok_spec, spec_edf, spec_efd, spec_edf), check_vma=False)
```

```python
import functools

import jax
import jax.numpy as jnp
from jax import lax
from jax.experimental import pallas as pl
from jax.experimental.pallas import tpu as pltpu
from jax.sharding import PartitionSpec as P

MESH = pl.DeviceIdType.MESH
BF = jnp.bfloat16
F32 = jnp.float32
ANY = pl.BlockSpec(memory_space=pl.ANY)
VM = pl.BlockSpec(memory_space=pltpu.VMEM)
VLIM = 62 * 1024 * 1024
GROUPS = (2, 6)
DROPPED = -4096.0
LANES = 128
EXP = 8
NT = (((1,), (1,)), ((), ()))
TN = (((0,), (0,)), ((), ()))


def params(collective_id=None):
    if collective_id is None:
        return pltpu.CompilerParams(vmem_limit_bytes=VLIM)
    return pltpu.CompilerParams(collective_id=collective_id, has_side_effects=True, vmem_limit_bytes=VLIM)


def cost(gflop, mbytes):
    return pl.CostEstimate(flops=gflop * 10**9, bytes_accessed=mbytes * 10**6, transcendentals=0)


def capacity_of(tok_rows, top_k, experts):
    return 8 * ((5 * tok_rows * top_k + 32 * experts - 1) // (32 * experts))


def dot(a, b):
    return jnp.dot(a, b, preferred_element_type=F32)


def hot_bf(sel):
    return jnp.where(sel, 1.0, 0.0).astype(BF)


def iota(shape, dim):
    return lax.broadcasted_iota(jnp.int32, shape, dim).astype(F32)


class Place:
    def __init__(self):
        me = lax.axis_index('ep')
        z = lax.axis_index('fsdp')
        self.me = me
        self.core = lax.rem(me, 2)
        self.other = 1 - self.core
        self.partner = me + 1 - 2 * self.core
        self.chip = lax.div(me, 2)
        self.to_x = 1 - 2 * lax.rem(self.chip, 2)
        self.to_y = 2 - 4 * lax.div(self.chip, 2)
        self.chip_x = self.chip + self.to_x
        self.chip_y = self.chip + self.to_y
        self.chip_d = self.chip_x + self.to_y
        self.dev_x = (z, 2 * self.chip_x + self.core)
        self.dev_y = (z, 2 * self.chip_y + self.core)
        self.dev_d = (z, 2 * self.chip_d + self.core)
        self.dev_c = (z, self.partner)

    def greet(self, *devices):
        barrier = pltpu.get_barrier_semaphore()
        for dev in devices:
            pl.semaphore_signal(barrier, inc=1, device_id=dev, device_id_type=MESH)
        pl.semaphore_wait(barrier, len(devices))


def rcopy(src, dst, sems, i, dev):
    return pltpu.make_async_remote_copy(src_ref=src, dst_ref=dst, send_sem=sems[0].at[i], recv_sem=sems[1].at[i], device_id=dev, device_id_type=MESH)


def arrive(ref, sems, i, dev):
    rcopy(ref, ref, sems, i, dev).wait_recv()


def gather_rows_kernel(capacity, x_ref, dy_ref, meta_ref, rows, pos_ref, gate_ref, post_ref, ids_ref, tg, mg, hot_a, hot_b, tri, stage, s_x, r_x, s_y, r_y, s_c, r_c, s_ax, r_ax, s_ay, r_ay, s_fx, r_fx, s_fy, r_fy, s_fa, r_fa, s_fb, r_fb, s_l, s_s):
    at = Place()
    tok = x_ref.shape[1]
    half = tok // 2
    by_x, by_y, by_c, relay_x, relay_y = (s_x, r_x), (s_y, r_y), (s_c, r_c), (s_ax, r_ax), (s_ay, r_ay)
    fwd_x, fwd_y, fwd_a, fwd_b = (s_fx, r_fx), (s_fy, r_fy), (s_fa, r_fa), (s_fb, r_fb)
    chunks = range(5)

    def slot_of(core, chip):
        return core * 4 + chip

    def own(k):
        if k == 0:
            return meta_ref
        return (dy_ref, x_ref)[k % 2].at[(k - 1) // 2]

    def block(k, slot):
        if k == 0:
            return mg.at[slot]
        return tg.at[(k - 1) % 2, slot, (k - 1) // 2]

    def part(k, slot, h):
        return block(k, slot).at[pl.ds(h * half, half)]

    slot = slot_of(at.core, at.chip)
    slot_x = slot_of(at.core, at.chip_x)
    slot_y = slot_of(at.core, at.chip_y)
    slot_d = slot_of(at.core, at.chip_d)

    def side_hops(k):
        return (
            (part(k, slot_x, 0), part(k, slot_x, 0), relay_y, k, at.dev_y),
            (block(k, slot_x), block(k, slot_x), fwd_x, k, at.dev_c),
            (part(k, slot_y, 1), part(k, slot_y, 1), relay_x, k, at.dev_x),
            (block(k, slot_y), block(k, slot_y), fwd_y, k, at.dev_c),
        )

    def corner_hops(k):
        return ((part(k, slot_d, 0), part(k, slot_d, 0), fwd_a, k, at.dev_c), (part(k, slot_d, 1), part(k, slot_d, 1), fwd_b, k, at.dev_c))

    def own_hops(k):
        return tuple((own(k), block(k, slot), sems, k, dev) for sems, dev in ((by_c, at.dev_c), (by_x, at.dev_x), (by_y, at.dev_y)))

    def meta_hops():
        return tuple((meta_ref, mg.at[slot], sems, 0, dev) for sems, dev in ((relay_x, at.dev_d), (by_x, at.dev_x), (by_y, at.dev_y), (by_c, at.dev_c)))

    def meta_shares():
        return tuple((mg.at[src], mg.at[src], sems, 0, at.dev_c) for src, sems in ((slot_x, fwd_x), (slot_y, fwd_y), (slot_d, fwd_a)))

    def send(hops):
        for hop in hops:
            rcopy(*hop).start()

    def pass_on(k):
        hops = side_hops(k)
        arrive(block(k, slot_x), by_x, k, at.dev_x)
        send(hops[:2])
        arrive(block(k, slot_y), by_y, k, at.dev_y)
        send(hops[2:])
        arrive(block(k, slot_of(at.other, at.chip_x)), fwd_x, k, at.dev_c)
        arrive(block(k, slot_of(at.other, at.chip_y)), fwd_y, k, at.dev_c)

    def pass_on_corner(k):
        hops = corner_hops(k)
        far = slot_of(at.other, at.chip_d)
        arrive(part(k, slot_d, 0), relay_y, k, at.dev_y)
        send(hops[:1])
        arrive(part(k, slot_d, 1), relay_x, k, at.dev_x)
        send(hops[1:])
        arrive(part(k, far, 0), fwd_a, k, at.dev_c)
        arrive(part(k, far, 1), fwd_b, k, at.dev_c)

    local = [pltpu.make_async_copy(own(k), block(k, slot), s_l.at[k]) for k in chunks]
    for copy in local:
        copy.start()
    at.greet(at.dev_x, at.dev_y, at.dev_d, at.dev_c)
    send(meta_hops())
    for k in chunks[1:]:
        send(own_hops(k))

    tri[...] = hot_bf(iota((tok, tok), 0) < iota((tok, tok), 1))
    for copy in local:
        copy.wait()
    arrive(mg.at[slot_of(at.other, at.chip)], by_c, 0, at.dev_c)
    shared = meta_shares()
    for n, (src, sems, dev) in enumerate(((slot_x, by_x, at.dev_x), (slot_y, by_y, at.dev_y), (slot_d, relay_x, at.dev_d))):
        arrive(mg.at[src], sems, 0, dev)
        send(shared[n:n + 1])
    for chip, sems in ((at.chip_x, fwd_x), (at.chip_y, fwd_y), (at.chip_d, fwd_a)):
        arrive(mg.at[slot_of(at.other, chip)], sems, 0, at.dev_c)
    sub = iota((EXP, tok), 0)

    def hot_of(src, mb, device):
        ids = mg[src, 0, mb]
        vals = mg[src, 1, mb]
        want = sub + (device * EXP).astype(F32)
        hot = jnp.zeros((EXP, tok), F32)
        gate = hot
        for j in range(ids.shape[0]):
            sel = ids[j:j + 1, :] == want
            hot = jnp.where(sel, 1.0, hot)
            gate = jnp.where(sel, vals[j:j + 1, :], gate)
        return hot, gate

    @pl.loop(0, 16)
    def _(i):
        hot, gate = hot_of(lax.div(i, 2), lax.rem(i, 2), at.me)
        hot_a[pl.ds(pl.multiple_of(i * EXP, EXP), EXP), :] = hot
        gate_ref[i] = gate

    @pl.loop(0, 8)
    def _(i):
        src, mb = slot_of(at.core, lax.div(i, 2)), lax.rem(i, 2)
        row = pl.multiple_of(i * 2 * EXP, EXP)
        hot_b[pl.ds(row, EXP), :] = hot_of(src, mb, at.me)[0]
        hot_b[pl.ds(row + EXP, EXP), :] = hot_of(src, mb, at.partner)[0]
        ids_ref[i] = mg[src, 0, mb]

    def place_of(hot):
        before = dot(hot.astype(BF), tri[...])
        keep = jnp.logical_and(hot > 0.5, before < capacity)
        return jnp.where(keep, before, DROPPED)

    pos_ref[...] = place_of(hot_a[...]).reshape(pos_ref.shape)
    post_ref[...] = jnp.transpose(place_of(hot_b[...]))

    place = iota((capacity, tok), 0)
    per = EXP // 2

    def stored(b, kind, i):
        return pltpu.make_async_copy(stage.at[b], rows.at[kind, :, i], s_s.at[b])

    @pl.loop(0, 32)
    def _(t):
        u = lax.div(t, 8)
        first = lax.div((3 - u) * (2 - u) * (1 - u), 6)
        last = lax.div(u * (u - 1) * (u - 2), 6)
        sides = 1 - first - last

        @pl.when(t == 0)
        def _():
            for k in chunks[1:]:
                arrive(block(k, slot_of(at.other, at.chip)), by_c, k, at.dev_c)

        for k in chunks[1:]:

            @pl.when(t == 4 + 4 * k)
            def _():
                pass_on(k)

            @pl.when(t == 22 + 2 * k)
            def _():
                pass_on_corner(k)

        k0 = first * lax.div(t, 2) + sides * (lax.div(t, 4) - 2) + last * (lax.div(t, 2) - 12)
        kind, mb = lax.rem(k0, 2), lax.div(k0, 2)
        far = (first + last) * lax.rem(t, 2) + sides * lax.div(lax.rem(t, 4), 2)
        core = at.core + far * (1 - 2 * at.core)
        odd = lax.rem(t, 2)
        chip = at.chip + sides * ((1 - odd) * at.to_x + odd * at.to_y) + last * (at.to_x + at.to_y)
        src = slot_of(core, chip)
        i = src * 2 + mb
        b = lax.rem(t, 2)

        @pl.when(t >= 2)
        def _():
            stored(b, kind, i).wait()

        pos = pos_ref[i]
        for h in range(0, EXP, per):
            hot = jnp.concatenate([hot_bf(pos[e:e + 1, :] == place) for e in range(h, h + per)], axis=0)
            stage[b, h:h + per] = dot(hot, tg[kind, src, mb]).astype(BF).reshape(per, capacity, -1)
        stored(b, kind, i).start()

    for b in range(2):
        stored(b, 0, b).wait()
    for hop in meta_hops() + meta_shares():
        rcopy(*hop).wait_send()
    for k in chunks[1:]:
        for hop in own_hops(k) + side_hops(k) + corner_hops(k):
            rcopy(*hop).wait_send()


def gather_rows(x_in, dy_out, meta, capacity):
    micro, tok, width = x_in.shape
    dma = pltpu.SemaphoreType.DMA
    table = jax.ShapeDtypeStruct((16, EXP, tok), F32)
    hots = pltpu.VMEM((LANES, tok), F32)
    return pl.pallas_call(
        functools.partial(gather_rows_kernel, capacity),
        out_shape=(jax.ShapeDtypeStruct((2, EXP, 16, capacity, width), BF), table, table, jax.ShapeDtypeStruct((tok, LANES), F32), jax.ShapeDtypeStruct((8, EXP, tok), F32)),
        in_specs=[ANY] * 3,
        out_specs=(ANY, VM, VM, VM, VM),
        scratch_shapes=[pltpu.VMEM((2, 8, micro, tok, width), BF), pltpu.VMEM((8,) + meta.shape, F32), hots, hots, pltpu.VMEM((tok, tok), BF), pltpu.VMEM((2, EXP, capacity, width), BF)] + [dma((5,))] * 19 + [dma((2,))],
        name='gather_rows',
        compiler_params=params(0),
        cost_estimate=cost(100, 80),
    )(x_in, dy_out, meta)


def expert_kernel(first, pos_ref, gate_ref, xr_ref, dyr_ref, w1_ref, w3_ref, w2_ref, dxr_ref, dg_ref, gw_ref, acc13, acc2):
    m = pl.program_id(1)
    e = pl.program_id(0) + first
    blocks, capacity, width = xr_ref.shape[2:]
    tok = pos_ref.shape[2]
    rows = blocks * capacity
    x = xr_ref[0, 0].reshape(rows, width)
    dy = dyr_ref[0, 0].reshape(rows, width)
    ff = w1_ref.shape[3]
    w13 = jnp.concatenate([w1_ref[:, 0].reshape(width, ff), w3_ref[:, 0].reshape(width, ff)], axis=1)
    w2 = jnp.concatenate([w2_ref[z, 0] for z in range(4)], axis=1)
    place = iota((capacity, tok), 0)
    pos_rows = [pos_ref[m * blocks + b, pl.ds(e, 1), :] for b in range(blocks)]
    q = jnp.concatenate([jnp.sum(jnp.where(pos_rows[b] == place, gate_ref[m * blocks + b, pl.ds(e, 1), :], 0.0), axis=1, keepdims=True) for b in range(blocks)], axis=0)
    g = (q * dy.astype(F32)).astype(BF)
    h = dot(x, w13)
    dyw = lax.dot_general(dy, w2, NT, preferred_element_type=F32)
    da = lax.dot_general(g, w2, NT, preferred_element_type=F32)
    h1 = h[:, :ff]
    h3 = h[:, ff:]
    sig = jax.nn.sigmoid(h1)
    s = h1 * sig
    act = (s * h3).astype(BF)
    dg = jnp.sum(act.astype(F32) * dyw, axis=1, keepdims=True)
    dh3 = (da * s).astype(BF)
    dh1 = (da * h3 * sig * (1.0 + h1 * (1.0 - sig))).astype(BF)
    dh = jnp.concatenate([dh1, dh3], axis=1)
    dx = lax.dot_general(dh, w13, NT, preferred_element_type=F32).astype(BF)
    dxr_ref[0] = dx.reshape(blocks, capacity, width)
    for b in range(blocks):
        col = dg[b * capacity:(b + 1) * capacity]
        dg_ref[0, pl.ds(m * blocks + b, 1), :] = jnp.sum(jnp.where(pos_rows[b] == place, col, 0.0), axis=0, keepdims=True)
    g13 = lax.dot_general(x, dh, TN, preferred_element_type=F32)
    g2 = lax.dot_general(act, g, TN, preferred_element_type=F32)

    @pl.when(m == 0)
    def _():
        acc13[...] = g13
        acc2[...] = g2

    @pl.when(m > 0)
    def _():
        acc13[...] += g13
        acc2[...] += g2

    @pl.when(m == pl.num_programs(1) - 1)
    def _():
        for z in range(4):
            cols = slice(z * LANES, z * LANES + LANES)
            for c in range(4):
                gw_ref[z, c // 2, 0, LANES * (c % 2):LANES * (c % 2) + LANES] = acc13[cols, c * LANES:c * LANES + LANES]
            gw_ref[z, 2, 0] = acc2[:, cols]


def expert_pass(first, count, pos, gate, rows, w_one, w_three, w_two):
    blocks = 8
    pairs, capacity, width = rows.shape[2:]
    tok = pos.shape[2]

    def row_spec(kind):
        return pl.BlockSpec((1, 1, blocks, capacity, width), lambda e, m: (kind, e + first, m, 0, 0))

    def w_spec(w):
        return pl.BlockSpec((w.shape[0], 1) + w.shape[2:], lambda e, m: (0, e + first, 0, 0))

    weights = w_two.shape[2:]
    fold = (4, 3, 1) + weights
    return pl.pallas_call(
        functools.partial(expert_kernel, first),
        grid=(count, pairs // blocks),
        out_shape=(jax.ShapeDtypeStruct((count, pairs, capacity, width), BF), jax.ShapeDtypeStruct((count, pairs, tok), F32), jax.ShapeDtypeStruct((4, 3, count) + weights, F32)),
        in_specs=[VM, VM, row_spec(0), row_spec(1), w_spec(w_one), w_spec(w_three), w_spec(w_two)],
        out_specs=(pl.BlockSpec((1, blocks, capacity, width), lambda e, m: (e, m, 0, 0)), pl.BlockSpec((1, pairs, tok), lambda e, m: (e, 0, 0)), pl.BlockSpec(fold, lambda e, m: (0, 0, e, 0, 0))),
        scratch_shapes=[pltpu.VMEM((width, width), F32), pltpu.VMEM((weights[0], width), F32)],
        name='expert_pass',
        compiler_params=params(),
        cost_estimate=cost(6 * count, 10 * count),
    )(pos, gate, rows, rows, w_one, w_three, w_two)


def reduce_kernel(groups, *refs):
    post_ref, ids_ref = refs[:2]
    rows, dgs = refs[2:2 + groups], refs[2 + groups:2 + 2 * groups]
    dx_ref, dgate_ref, hot, near, far, far_dg, q_ref, g_ref, in_x, in_y, last_x, last_y, g_in, g_last, s_h, s_f, r_f, s_d, r_d, s_x, r_x, s_y, r_y, s_2x, r_2x, s_2y, r_2y, s_g, r_g = refs[2 + 2 * groups:]
    at = Place()
    capacity, width = near.shape[2:]
    tok = post_ref.shape[0]
    half = tok // 2
    upper = pl.ds(0, half)
    lower = pl.ds(half, half)
    swap, swap_dg, hop_x, hop_y, hop_2x, hop_2y, hop_g = (s_f, r_f), (s_d, r_d), (s_x, r_x), (s_y, r_y), (s_2x, r_2x), (s_2y, r_2y), (s_g, r_g)
    firsts = [sum(ref.shape[0] for ref in rows[:n]) for n in range(groups)]

    def span(n):
        return pl.ds(firsts[n], rows[n].shape[0])

    def pair_of(t):
        p, mb = lax.div(t, 2), lax.rem(t, 2)
        return (at.chip + (1 - lax.div(p, 2)) * at.to_x + (1 - lax.rem(p, 2)) * at.to_y) * 2 + mb

    def loads(t):
        b = lax.rem(t, 2)
        return [pltpu.make_async_copy(rows[n].at[:, at.core * 8 + pair_of(t)], near.at[b, span(n)], s_h.at[b, n]) for n in range(groups)]

    def swaps(t):
        return [rcopy(rows[n].at[:, at.other * 8 + pair_of(t)], far.at[t, span(n)], swap, (n, t), at.dev_c) for n in range(groups)]

    def swaps_dg():
        return [rcopy(dgs[n].at[:, pl.ds(pl.multiple_of(at.other * 8, 8), 8)], far_dg.at[span(n)], swap_dg, n, at.dev_c) for n in range(groups)]

    def send(src, dst, sems, i, dev):
        rcopy(src, dst, sems, i, dev).start()

    def sent(src, dst, sems, i, dev):
        rcopy(src, dst, sems, i, dev).wait_send()

    def first_hops(p, mb):
        hops = []
        if p < 2:
            hops.append((q_ref.at[p, mb, upper], in_x.at[mb, 1 - p], hop_x, 2 * mb + 1 - p, at.dev_x))
        if p % 2 == 0:
            hops.append((q_ref.at[p, mb, lower], in_y.at[mb, 1 - p // 2], hop_y, 2 * mb + 1 - p // 2, at.dev_y))
        return hops

    def gate_hop(p):
        return (g_ref.at[p], g_in.at[1 - p], hop_g, 1 - p, at.dev_x)

    for copy in loads(0):
        copy.start()
    at.greet(at.dev_x, at.dev_y, at.dev_c)

    @pl.loop(0, 8)
    def _(t):
        for copy in swaps(t):
            copy.start()

        @pl.when(t == 0)
        def _():
            for copy in swaps_dg():
                copy.start()

    lane = iota((tok, LANES), 1)
    tiles = 2 * EXP * capacity // LANES

    @pl.loop(0, 8)
    def _(t):
        p, mb = lax.div(t, 2), lax.rem(t, 2)
        i = pair_of(t)

        @pl.when(t < 7)
        def _():
            for copy in loads(t + 1):
                copy.start()

        post = pltpu.roll(post_ref[...], lax.rem(LANES - i * 2 * EXP, LANES), 1)
        for k in range(tiles):
            col = k * LANES
            lo = col // capacity
            sel = post[:, lo:lo + 1] == lane + (col - lo * capacity)
            for e in range(lo + 1, (col + LANES - 1) // capacity + 1):
                sel = jnp.logical_or(sel, post[:, e:e + 1] == lane + (col - e * capacity))
            hot[:, col:col + LANES] = hot_bf(sel)
        for copy in loads(t):
            copy.wait()
        for copy in swaps(t):
            copy.wait_recv()

        @pl.when(t == 0)
        def _():
            for copy in swaps_dg():
                copy.wait_recv()

        rows_near = near[mb].reshape(EXP * capacity, width)
        rows_far = far[t].reshape(EXP * capacity, width)
        q_ref[p, mb] = dot(hot[...], jnp.concatenate([rows_near, rows_far], axis=0))
        ids = ids_ref[i]
        total = jnp.zeros(ids.shape, F32)
        for n in range(groups):
            for c in range(rows[n].shape[0]):
                e = firsts[n] + c
                mine = dgs[n][c, pl.ds(at.core * 8 + i, 1), :]
                total = jnp.where(ids == (at.me * EXP + e).astype(F32), mine, total)
                total = jnp.where(ids == (at.partner * EXP + e).astype(F32), far_dg[e, pl.ds(i, 1), :], total)
        g_ref[p, mb] = total
        for c in range(3):

            @pl.when(p == c)
            def _():
                for hop in first_hops(c, mb):
                    send(*hop)

        for c in range(2):

            @pl.when(t == 2 * c + 1)
            def _():
                send(*gate_hop(c))

    arrive(g_in.at[1], hop_g, 1, at.dev_x)
    g_in[1] += g_ref[2]
    gate_last = (g_in.at[1], g_last, hop_g, 2, at.dev_y)
    send(*gate_last)

    def last_hops(mb):
        return ((in_x.at[mb, 1], last_y.at[mb], hop_2y, mb, at.dev_y), (in_y.at[mb, 1], last_x.at[mb], hop_2x, mb, at.dev_x))

    for mb in range(2):
        hops = last_hops(mb)
        arrive(in_x.at[mb, 1], hop_x, 2 * mb + 1, at.dev_x)
        in_x[mb, 1] += q_ref[2, mb, upper]
        send(*hops[0])
        arrive(in_y.at[mb, 1], hop_y, 2 * mb + 1, at.dev_y)
        in_y[mb, 1] += q_ref[1, mb, lower]
        send(*hops[1])
    arrive(g_in.at[0], hop_g, 0, at.dev_x)
    arrive(g_last, hop_g, 2, at.dev_y)
    dgate_ref[...] = g_ref[3] + g_in[0] + g_last[...]
    for mb in range(2):
        arrive(in_x.at[mb, 0], hop_x, 2 * mb, at.dev_x)
        arrive(in_y.at[mb, 0], hop_y, 2 * mb, at.dev_y)
        q_ref[3, mb, upper] += in_x[mb, 0]
        q_ref[3, mb, lower] += in_y[mb, 0]
    for mb in range(2):
        arrive(last_y.at[mb], hop_2y, mb, at.dev_y)
        dx_ref[mb, upper] = (q_ref[3, mb, upper] + last_y[mb]).astype(BF)
        arrive(last_x.at[mb], hop_2x, mb, at.dev_x)
        dx_ref[mb, lower] = (q_ref[3, mb, lower] + last_x[mb]).astype(BF)
    for mb in range(2):
        sent(*gate_hop(mb))
        for c in range(3):
            for hop in first_hops(c, mb):
                sent(*hop)
        for hop in last_hops(mb):
            sent(*hop)
    sent(*gate_last)
    for copy in swaps_dg():
        copy.wait_send()

    @pl.loop(0, 8)
    def _(t):
        for copy in swaps(t):
            copy.wait_send()


def reduce_chips(post, ids, rows, dgs):
    groups = len(rows)
    capacity, width = rows[0].shape[2:]
    tok = post.shape[0]
    top_k = ids.shape[1]
    half = tok // 2
    dma = pltpu.SemaphoreType.DMA
    vm = pltpu.VMEM
    return pl.pallas_call(
        functools.partial(reduce_kernel, groups),
        out_shape=(jax.ShapeDtypeStruct((2, tok, width), BF), jax.ShapeDtypeStruct((2, top_k, tok), F32)),
        in_specs=[VM, VM] + [ANY] * groups + [VM] * groups,
        out_specs=(VM, VM),
        scratch_shapes=[vm((tok, 2 * EXP * capacity), BF), vm((2, EXP, capacity, width), BF), vm((8, EXP, capacity, width), BF), vm((EXP, 8, tok), F32), vm((4, 2, tok, width), F32), vm((4, 2, top_k, tok), F32)]
        + [vm((2, 2, half, width), F32)] * 2 + [vm((2, half, width), F32)] * 2 + [vm((2, 2, top_k, tok), F32), vm((2, top_k, tok), F32), dma((2, groups))]
        + [dma((groups, 8))] * 2 + [dma((groups,))] * 2 + [dma((4,))] * 4 + [dma((2,))] * 4 + [dma((3,))] * 2,
        name='reduce_chips',
        compiler_params=params(2),
        cost_estimate=cost(100, 40),
    )(post, ids, *rows, *dgs)


def solution(mesh):
    ep_size = mesh.shape['ep']
    tok_spec = P(None, ('fsdp', 'ep'), None)
    spec_edf = P('ep', 'fsdp', None)
    spec_efd = P('ep', None, 'fsdp')

    def unfold(g):
        halves = g.reshape(g.shape[0], -1, LANES, LANES)
        return jnp.swapaxes(halves, 1, 2).reshape(g.shape[0], LANES, -1)

    def local_step(x_in, dy_out, expert_idx, gate_prob, w_one, w_two, w_three):
        micro, tok, width = x_in.shape
        top_k = expert_idx.shape[2]
        local_experts = w_one.shape[0]
        capacity = capacity_of(tok, top_k, local_experts * ep_size)
        w_all = [lax.all_gather(w, 'fsdp', axis=0, tiled=False) for w in (w_one, w_three, w_two)]
        meta = jnp.stack([jnp.transpose(expert_idx, (0, 2, 1)).astype(F32), jnp.transpose(gate_prob, (0, 2, 1))])
        rows, pos, gate, post, ids = gather_rows(x_in, dy_out, meta, capacity)
        dx_rows, dgs, grads = [], [], []
        for count in GROUPS:
            first = sum(r.shape[0] for r in dx_rows)
            r, d, g = expert_pass(first, count, pos, gate, rows, *w_all)
            dx_rows.append(r)
            dgs.append(d)
            grads.append(lax.psum_scatter(g, 'fsdp', scatter_dimension=0, tiled=False))
        dx, dgate = reduce_chips(post, ids, dx_rows, dgs)
        grad = jnp.concatenate(grads, axis=1)
        return dx, jnp.transpose(dgate, (0, 2, 1)), unfold(grad[0]), grad[2], unfold(grad[1])

    return jax.shard_map(local_step, mesh=mesh, in_specs=(tok_spec, tok_spec, tok_spec, tok_spec, spec_edf, spec_efd, spec_edf), out_specs=(tok_spec, tok_spec, spec_edf, spec_efd, spec_edf), check_vma=False)
```
